32 devices in a mesh: act: 4 (over y, x), virt: 8 (over z, core).
Axes of the slice: x: 2, y: 2, z: 4, core: 2. Of those that a mesh axis runs over, the one named last changes fastest.
Arguments:
- amplitudes: bfloat16 [400, 640, 640], P('act', 'virt'), may hold values from -6 to 6
- virtual_fock_block: bfloat16 [640, 640], replicated, may hold values from -1 to 3.1, as said below
- metric: bfloat16 [400, 400], replicated, may hold values from -3.5 to 3.5, as said below
- active_block: bfloat16 [400, 400], replicated, may hold values from -0.3125 to 0.3125
Outputs:
- residual_vec: bfloat16 [400, 640, 640], P('act', 'virt')
- rayleigh: float32 [], replicated
- res_norm: float32 [], replicated
The draws below stay inside these ranges and needn't reach their ends.
Inputs may be any that keep to these rules, and one draw needn't show every extreme that they name: `virtual_fock_block`: symmetric. `metric`: symmetric positive definite.
All inputs are finite; a program needn't handle non-finite values.
Results may differ from the reference program's by a relative error of at most 0.0099.
Values may be sent and summed in bfloat16 or wider, within the bound.
A program may use at most 192 MiB of HBM per device.

```python
import jax
import jax.numpy as jnp
from jax import lax

NV = 640
TU = 400


def draw_virtual_fock_block(key, part):
    leading_key, second_key = jax.random.split(jax.random.fold_in(key, 11))
    energies = jax.random.uniform(leading_key, (NV,), jnp.float32, 0.5, 3.0)
    coupling = jax.random.uniform(second_key, (NV, NV), jnp.float32, -1.0, 1.0) * 1.7
    coupling = (coupling + coupling.T) * (0.35 / math_sqrt(NV))
    coupling = coupling * (1.0 - jnp.eye(NV, dtype=jnp.float32))
    return (jnp.diag(energies) + coupling).astype(jnp.bfloat16)


def math_sqrt(value):
    return float(value) ** 0.5


def draw_metric(key, part):
    leading_key = jax.random.fold_in(jax.random.fold_in(key, 23), 0)
    factor = jax.random.uniform(leading_key, (TU, TU), jnp.float32, -1.7, 1.7)
    product = jnp.dot(factor, factor.T, precision=lax.Precision.HIGHEST) / TU
    return (0.5 * jnp.eye(TU, dtype=jnp.float32) + product).astype(jnp.bfloat16)


def level_of(own_key, extent, pieces, least, top_value):
    level, own = 1.0, jax.random.fold_in(own_key, 6)
    for axis_at, shards_of in pieces:
        heights = jnp.exp(jax.random.uniform(jax.random.fold_in(own, axis_at), (shards_of,), jnp.float32, least / len(pieces), top_value / len(pieces)))
        level = level * jnp.repeat(heights, extent[axis_at] // shards_of).reshape([-1 if axis == axis_at else 1 for axis in range(len(extent))])
    return level


def noise(key, shape, scale, most, shards=(), held_as=jnp.bfloat16):
    drawn = jax.random.normal(key, shape, jnp.float32) * scale
    if len(shards) > 0:
        drawn = level_of(key, shape, shards, -0.22, 0.18) * drawn
    return jnp.clip(drawn, min=-most, max=most).astype(held_as)


def setup_inputs(seed: int = 0) -> dict:
    keys = jax.random.split(jax.random.key(seed), 5)
    amplitudes = noise(keys[0], (TU, NV, NV), 1.0, 6.0, ((0, 4), (1, 8)))
    virtual_fock_block = draw_virtual_fock_block(jax.random.fold_in(keys[4], 71), 0)
    metric = draw_metric(jax.random.fold_in(keys[4], 71), 0)
    active_block = noise(keys[3], (TU, TU), TU ** -0.5, 0.3125)
    return dict(amplitudes=amplitudes, virtual_fock_block=virtual_fock_block, metric=metric, active_block=active_block)


def reference(amplitudes, virtual_fock_block, metric, active_block):
    broadened_fock = virtual_fock_block.astype(jnp.float32)
    block_of_rows = 32
    blocks_count = NV // block_of_rows
    indices = jnp.arange(blocks_count, dtype=jnp.int32)

    def metric_rows(index):
        start = (index * block_of_rows).astype(jnp.int32)
        trial_rows = lax.dynamic_slice_in_dim(amplitudes, start, block_of_rows, 1)
        flat_trial = trial_rows.reshape(TU, block_of_rows * NV)
        weighted_rows = jnp.dot(metric, flat_trial, preferred_element_type=jnp.float32)
        return weighted_rows.astype(jnp.bfloat16).reshape(TU, block_of_rows, NV)

    half_blocks = lax.map(metric_rows, indices)
    weighted_half = jnp.moveaxis(half_blocks, 0, 1).reshape(TU, NV, NV)

    def left_group(group_rows):
        return jnp.einsum("ac,tcb->tab", broadened_fock, group_rows.astype(jnp.float32)).astype(jnp.bfloat16)

    left_portion = lax.map(left_group, weighted_half.reshape(TU // 4, 4, NV, NV)).reshape(TU, NV, NV)

    def project(index):
        start = (index * block_of_rows).astype(jnp.int32)
        trial_rows = lax.dynamic_slice_in_dim(amplitudes, start, block_of_rows, 1)
        halved_rows = lax.dynamic_slice_in_dim(weighted_half, start, block_of_rows, 1)
        left_rows = lax.dynamic_slice_in_dim(left_portion, start, block_of_rows, 1)
        flat_trial = trial_rows.reshape(TU, block_of_rows * NV)
        rightside_rows = jnp.einsum("wuv,vq->wuq", halved_rows.astype(jnp.float32), broadened_fock)
        sigma_rows = left_rows.astype(jnp.float32).reshape(TU, block_of_rows * NV) + rightside_rows.reshape(TU, block_of_rows * NV) + jnp.dot(active_block, flat_trial, preferred_element_type=jnp.float32)
        weighted_rows = jnp.dot(metric, flat_trial, preferred_element_type=jnp.float32)
        return sigma_rows, weighted_rows, flat_trial.astype(jnp.float32)

    def intersect(index):
        sigma_rows, weighted_rows, trial_wide = project(index)
        return jnp.sum(trial_wide * sigma_rows), jnp.sum(trial_wide * weighted_rows)

    numer_parts, denom_parts = lax.map(intersect, indices)
    numerator = jnp.sum(numer_parts)
    denominator = jnp.sum(denom_parts)
    rayleigh = numerator / denominator

    def finish(index):
        sigma_rows, weighted_rows, trial_wide = project(index)
        resid = sigma_rows - rayleigh * weighted_rows
        return resid.astype(jnp.bfloat16).reshape(TU, block_of_rows, NV), jnp.sum(resid * resid)

    resid_blocks, square_parts = lax.map(finish, indices)
    residual_vec = jnp.moveaxis(resid_blocks, 0, 1).reshape(TU, NV, NV)
    res_norm = jnp.sum(square_parts) / denominator
    return residual_vec, rayleigh, res_norm
```

```python
import functools

import jax
import jax.numpy as jnp
from jax import lax
from jax.experimental import pallas as pl
from jax.experimental.pallas import tpu as pltpu
from jax.sharding import PartitionSpec as P

MESH = pl.DeviceIdType.MESH
AHEAD = 4


HIGH = 16
SLOTS = 8
WINDOW = 8


def main_kernel(groups, peers, rows, cut, shift_ref, fock_ref, metric_ref, active_ref, trial_ref,
                trial_rows, image_rows, image_ref, front_ref, front_rows, left_ref, rest_rows, rest_ref,
                held_a, held_b, made_a, made_b, late_held, soon_held, front_held, late_image, soon_image,
                late_kept, soon_kept, rest_made, flat, turned, sems_a, sems_b, act_sems, loaded, stored):
    group, me = lax.axis_index("act"), lax.axis_index("virt")
    pairs, padded, width = trial_ref.shape
    rounds = held_a.shape[0]
    items = rows // groups
    chunks = padded // HIGH
    per_chunk = HIGH // groups
    soon, late = pl.ds(0, cut), pl.ds(cut, width - cut)

    barrier = pltpu.get_barrier_semaphore()
    for step in range(1, peers):
        pl.semaphore_signal(
            barrier, inc=1, device_id=(group, lax.rem(me + step, peers)), device_id_type=MESH)
    for step in range(1, groups):
        pl.semaphore_signal(
            barrier, inc=1, device_id=(lax.rem(group + step, groups), me), device_id_type=MESH)

    whole_rounds = pairs // peers
    spare = pairs % peers
    stride = peers // spare if spare and peers % spare == 0 else 1

    def pair_of(r, owner):
        return r * peers + owner - (r // whole_rounds) * (owner - owner // stride)

    def owns(r, owner):
        return (r // whole_rounds) * peers * lax.rem(owner, stride) + pair_of(r, owner) < pairs

    class Fock:
        def __init__(self, source, columns, held, made, target, sems):
            self.source, self.columns, self.held, self.made = source, columns, held, made
            self.target, self.sems, self.ring = target, sems, made.shape[0]

        def slab(self, t):
            return self.source.at[t, :, self.columns]

        def forward(self, r, peer):
            return pltpu.make_async_remote_copy(
                src_ref=self.slab(pair_of(r, peer)), dst_ref=self.held.at[r, me],
                send_sem=self.sems.at[0, r, peer], recv_sem=self.sems.at[1, r, me],
                device_id=(group, peer), device_id_type=MESH)

        def forward_own(self, r):
            return pltpu.make_async_copy(
                self.slab(pair_of(r, me)), self.held.at[r, me], self.sems.at[1, r, me])

        def arrival(self, r, peer):
            return pltpu.make_async_remote_copy(
                src_ref=self.held.at[r, me], dst_ref=self.held.at[r, peer],
                send_sem=self.sems.at[0, r, peer], recv_sem=self.sems.at[1, r, peer],
                device_id=(group, peer), device_id_type=MESH)

        def backward(self, r, peer):
            return pltpu.make_async_remote_copy(
                src_ref=self.made.at[lax.rem(r, self.ring), peer], dst_ref=self.target.at[pair_of(r, me)],
                send_sem=self.sems.at[2, r, peer], recv_sem=self.sems.at[3, r, me],
                device_id=(group, peer), device_id_type=MESH)

        def backward_own(self, r):
            return pltpu.make_async_copy(
                self.made.at[lax.rem(r, self.ring), me], self.target.at[pair_of(r, me)], self.sems.at[3, r, me])

        def back_arrival(self, r, peer):
            return pltpu.make_async_remote_copy(
                src_ref=self.made.at[0, peer], dst_ref=self.target.at[pair_of(r, peer)],
                send_sem=self.sems.at[2, r, peer], recv_sem=self.sems.at[3, r, peer],
                device_id=(group, peer), device_id_type=MESH)

        def launch(self, r):
            for step in range(peers):
                peer = lax.rem(me + step, peers)

                @pl.when(owns(r, peer))
                def _(step=step, peer=peer):
                    if step == 0:
                        self.forward_own(r).start()
                    else:
                        self.forward(r, peer).start()

        def launch_first(self):
            def ahead(r, carry):
                self.launch(r)
                return carry

            lax.fori_loop(0, min(AHEAD, rounds), ahead, 0)

        def launch_next(self, r):
            @pl.when(r + AHEAD < rounds)
            def _():
                self.launch(r + AHEAD)

        def sent_back(self, r):
            for step in range(1, peers):
                self.backward(r, lax.rem(me + step, peers)).wait_send()

        def apply(self, r):
            @pl.when(r >= 1)
            def _():
                self.backward_own(r - 1).wait()

            @pl.when(owns(r, me))
            def _():
                self.forward_own(r).wait()
                for step in range(1, peers):
                    self.arrival(r, lax.rem(me + step, peers)).wait_recv()

                @pl.when(r >= self.ring)
                def _():
                    self.sent_back(r - self.ring)

                block = self.held[r].reshape(peers * padded, self.held.shape[3])
                product = jnp.dot(fock_ref[...], block, preferred_element_type=jnp.float32)
                self.made[lax.rem(r, self.ring)] = product.astype(jnp.bfloat16).reshape(
                    peers, padded, self.held.shape[3])
                self.backward_own(r).start()
                for step in range(1, peers):
                    self.backward(r, lax.rem(me + step, peers)).start()

        def settle(self):
            @pl.when(owns(rounds - 1, me))
            def _():
                self.backward_own(rounds - 1).wait()

            def landed(r, carry):
                for step in range(1, peers):
                    peer = lax.rem(me + step, peers)

                    @pl.when(owns(r, peer))
                    def _(peer=peer):
                        self.back_arrival(r, peer).wait_recv()

                return carry

            lax.fori_loop(0, rounds, landed, 0)

        def drain(self):
            def done(r, carry):
                for step in range(1, peers):
                    peer = lax.rem(me + step, peers)

                    @pl.when(owns(r, peer))
                    def _(peer=peer):
                        self.forward(r, peer).wait_send()

                return carry

            lax.fori_loop(0, rounds, done, 0)

            def back_done(r, carry):
                kept = (r + self.ring < rounds - 1) | ((r + self.ring == rounds - 1) & owns(rounds - 1, me))

                @pl.when(owns(r, me) & jnp.logical_not(kept))
                def _():
                    self.sent_back(r)

                return carry

            lax.fori_loop(0, rounds, back_done, 0)

    class Swap:
        def __init__(self, kind, source, target):
            self.kind, self.source, self.target = kind, source, target

        def send(self, i, peer):
            return pltpu.make_async_remote_copy(
                src_ref=self.source(i, peer), dst_ref=self.target(i, group),
                send_sem=act_sems.at[self.kind, 0, i, peer], recv_sem=act_sems.at[self.kind, 1, i, group],
                device_id=(peer, me), device_id_type=MESH)

        def own(self, i):
            return pltpu.make_async_copy(
                self.source(i, group), self.target(i, group), act_sems.at[self.kind, 1, i, group])

        def arrival(self, i, peer):
            return pltpu.make_async_remote_copy(
                src_ref=self.source(i, peer), dst_ref=self.target(i, peer),
                send_sem=act_sems.at[self.kind, 0, i, peer], recv_sem=act_sems.at[self.kind, 1, i, peer],
                device_id=(peer, me), device_id_type=MESH)

        def start(self, i):
            self.own(i).start()
            for step in range(1, groups):
                self.send(i, lax.rem(group + step, groups)).start()

        def wait_remote(self, i):
            for step in range(1, groups):
                self.arrival(i, lax.rem(group + step, groups)).wait_recv()

        def wait(self, i):
            self.own(i).wait()
            self.wait_remote(i)

        def sent(self, i):
            for step in range(1, groups):
                self.send(i, lax.rem(group + step, groups)).wait_send()

        def drain(self, first):
            def done(i, carry):
                self.sent(i)
                return carry

            lax.fori_loop(first, items, done, 0)

    def row(i, owner):
        return i * groups + owner

    def slot(i):
        return lax.rem(i, SLOTS)

    front = Fock(trial_ref, soon, held_a, made_a, front_ref, sems_a)
    back = Fock(image_ref, late, held_b, made_b, left_ref, sems_b)
    late_in = Swap(0, lambda i, p: trial_rows.at[row(i, p), :, late], lambda i, p: late_held.at[i, p])
    soon_in = Swap(1, lambda i, p: trial_rows.at[row(i, p), :, soon], lambda i, p: soon_held.at[i, p])
    late_out = Swap(2, lambda i, p: late_image.at[slot(i), p], lambda i, p: image_rows.at[row(i, p), :, late])
    soon_out = Swap(3, lambda i, p: soon_image.at[slot(i), p], lambda i, p: image_rows.at[row(i, p), :, soon])
    kept_out = Swap(4, lambda i, p: late_kept.at[i, p], lambda i, p: rest_rows.at[row(i, p), :, late])
    front_in = Swap(5, lambda i, p: front_rows.at[row(i, p)], lambda i, p: front_held.at[i, p])
    rest_out = Swap(6, lambda i, p: rest_made.at[slot(i), p], lambda i, p: rest_rows.at[row(i, p), :, soon])

    def run(low, high, work):
        def one(i, carry):
            work(i)
            return carry

        lax.fori_loop(low, high, one, 0)

    def strip(c):
        return pl.ds(pl.multiple_of(c * HIGH, HIGH), HIGH)

    def blocks(extent, work):
        def one(j, carry):
            work(pl.ds(pl.multiple_of(j * 128, 128), 128))
            return carry

        lax.fori_loop(0, extent // 128, one, 0)

    def to_rows(at, extent):
        def work(columns):
            turned[at, :, :, columns] = jnp.transpose(flat[at, :, :, columns], (1, 0, 2))

        blocks(extent, work)

    def to_flat(c, at, extent):
        def work(columns):
            block = jnp.transpose(turned[at, :, :, columns], (1, 0, 2))
            if padded != rows:
                place = c * HIGH + lax.broadcasted_iota(jnp.int32, block.shape, 1)
                block = jnp.where(place < rows, block, jnp.zeros_like(block))
            flat[at, :, :, columns] = block

        blocks(extent, work)

    def turn_back(c, source, target, columns, extent):
        load = pltpu.make_async_copy(
            source.at[strip(c), :, columns], turned.at[0, :, :, pl.ds(0, extent)], loaded.at[0])
        load.start()
        load.wait()
        to_flat(c, 0, extent)
        store = pltpu.make_async_copy(
            flat.at[0, :, :, pl.ds(0, extent)], target.at[:, strip(c), columns], stored.at[0])
        store.start()
        store.wait()

    def arrived(swap, c, work):
        run(c * per_chunk, jnp.minimum((c + 1) * per_chunk, items), work)

    def image_late(c):
        arrived(late_out, c, late_out.wait_remote)
        turn_back(c, image_rows, image_ref, late, width - cut)

    def image_soon(c):
        arrived(soon_out, c, soon_out.wait_remote)
        turn_back(c, image_rows, image_ref, soon, cut)

    def rest_late(c):
        arrived(kept_out, c, kept_out.wait)
        turn_back(c, rest_rows, rest_ref, late, width - cut)

    def rest_soon(c):
        arrived(rest_out, c, rest_out.wait_remote)
        turn_back(c, rest_rows, rest_ref, soon, cut)

    def mix(matrix_ref, held, i):
        total = jnp.dot(matrix_ref[0], held[i, 0], preferred_element_type=jnp.float32)
        for q in range(1, groups):
            total += jnp.dot(matrix_ref[q], held[i, q], preferred_element_type=jnp.float32)
        return total.reshape(groups, -1, total.shape[1])[:, :pairs]

    def weigh(i, taken, given, held, image, kept):
        taken.wait(i)

        @pl.when(i >= SLOTS)
        def _():
            given.sent(i - SLOTS)

        weighted = mix(metric_ref, held, i)
        half = weighted.astype(jnp.bfloat16)
        image[slot(i)] = half
        given.start(i)
        active = mix(active_ref, held, i) - shift_ref[0] * (weighted - half.astype(jnp.float32))
        kept[i] = active.astype(kept.dtype)
        given.own(i).wait()

    def feed(j):
        @pl.when(j < items)
        def _():
            late_in.start(j)

        @pl.when((j >= items) & (j < 2 * items))
        def _():
            soon_in.start(j - items)

    def weigh_late(i):
        feed(i + WINDOW)
        weigh(i, late_in, late_out, late_held, late_image, late_kept)

    def weigh_soon(i):
        feed(items + i + WINDOW)
        weigh(i, soon_in, soon_out, soon_held, soon_image, soon_kept)

    def combine(i):
        @pl.when(i + WINDOW < items)
        def _():
            front_in.start(i + WINDOW)

        front_in.wait(i)

        @pl.when(i >= SLOTS)
        def _():
            rest_out.sent(i - SLOTS)

        total = soon_kept[i].astype(jnp.float32) + mix(metric_ref, front_held, i)
        rest_made[slot(i)] = total.astype(jnp.bfloat16)
        rest_out.start(i)
        kept_out.start(i)
        rest_out.own(i).wait()

    def load_trial(c):
        return pltpu.make_async_copy(trial_ref.at[:, strip(c), :], flat.at[lax.rem(c, 2)], loaded.at[lax.rem(c, 2)])

    def store_rows(c):
        return pltpu.make_async_copy(turned.at[lax.rem(c, 2)], trial_rows.at[strip(c)], stored.at[lax.rem(c, 2)])

    def turn_trial(c):
        @pl.when(c < chunks)
        def _():
            load_trial(c).wait()
            to_rows(lax.rem(c, 2), width)
            store_rows(c).start()

        @pl.when(c + 2 < chunks)
        def _():
            load_trial(c + 2).start()

        @pl.when(c >= 1)
        def _():
            store_rows(c - 1).wait()
            run((c - 1) * per_chunk, jnp.minimum(c * per_chunk, min(WINDOW, items)), late_in.start)

    def turn_front(c):
        load = pltpu.make_async_copy(
            front_ref.at[:, strip(c), :], flat.at[0, :, :, soon], loaded.at[0])
        load.start()
        load.wait()
        to_rows(0, cut)
        store = pltpu.make_async_copy(turned.at[0, :, :, soon], front_rows.at[strip(c)], stored.at[0])
        store.start()
        store.wait()

    def count(value, most):
        return jnp.clip(value, 0, most)

    for c in range(min(2, chunks)):
        load_trial(c).start()
    pl.semaphore_wait(barrier, peers + groups - 2)
    front.launch_first()
    run(0, chunks + 1, turn_trial)
    run(items, WINDOW, feed)

    late_step = -(-items // max(1, rounds - 3))
    late_ticks = -(-items // late_step)

    def weighed_late(r):
        return count((r + 1) * late_step, items)

    def image_done(r):
        ready = count((r - 1) * late_step, items)
        return jnp.where(ready == items, chunks, ready // per_chunk)

    def weighed_early(r):
        return count((r + 1 - late_ticks) * late_step, items)

    def first_tick(r):
        front.launch_next(r)
        run(weighed_late(r - 1), weighed_late(r), weigh_late)
        run(weighed_early(r - 1), weighed_early(r), weigh_soon)
        run(image_done(r - 1), image_done(r), image_late)
        front.apply(r)

    run(0, rounds, first_tick)
    run(weighed_late(rounds - 1), items, weigh_late)
    run(image_done(rounds - 1), chunks, image_late)
    back.launch_first()

    soon_step = 2 * late_step
    begun = weighed_early(rounds - 1)

    def weighed_soon(r):
        return count(begun + (r + 1) * soon_step, items)

    def combined(r):
        return count((r - 3) * 5 // 2, items)

    def soon_done(r):
        return count(r - 3, chunks)

    def late_done(r):
        return count((r - 8) * 2, chunks)

    def second_tick(r):
        back.launch_next(r)
        run(weighed_soon(r - 1), weighed_soon(r), weigh_soon)

        @pl.when(r == 1)
        def _():
            front.settle()
            run(0, chunks, turn_front)
            run(0, min(WINDOW, items), front_in.start)

        run(combined(r - 1), combined(r), combine)
        run(soon_done(r - 1), soon_done(r), image_soon)
        run(late_done(r - 1), late_done(r), rest_late)
        back.apply(r)

    run(0, rounds, second_tick)
    last = rounds - 1
    run(weighed_soon(last), items, weigh_soon)
    run(combined(last), items, combine)
    run(soon_done(last), chunks, image_soon)
    run(late_done(last), chunks, rest_late)
    run(0, chunks, rest_soon)
    back.settle()
    front.drain()
    back.drain()
    late_in.drain(0)
    soon_in.drain(0)
    kept_out.drain(0)
    front_in.drain(0)
    for swap in (late_out, soon_out, rest_out):
        swap.drain(max(items - SLOTS, 0))


def sweep(groups, peers, rows, cut, shift, fock, metric, active, trial):
    pairs, padded, width = trial.shape
    items = rows // groups
    rounds = -(-pairs // peers)
    rest = width - cut
    ring = min(rounds, 6)
    tall = groups * items
    whole = pl.BlockSpec(memory_space=pltpu.VMEM)
    anywhere = pl.BlockSpec(memory_space=pl.ANY)
    half, dma = jnp.bfloat16, pltpu.SemaphoreType.DMA

    def made(*shape):
        return jax.ShapeDtypeStruct(shape, half)

    outs = pl.pallas_call(
        functools.partial(main_kernel, groups, peers, rows, cut),
        out_shape=[
            made(padded, pairs, width), made(padded, pairs, width), made(pairs, padded, width),
            made(pairs, padded, cut), made(padded, pairs, cut), made(pairs, padded, rest),
            made(padded, pairs, width), made(pairs, padded, width),
        ],
        in_specs=[pl.BlockSpec(memory_space=pltpu.SMEM)] + [whole] * 3 + [anywhere],
        out_specs=[anywhere] * 8,
        scratch_shapes=[
            pltpu.VMEM((rounds, peers, padded, cut), half),
            pltpu.VMEM((rounds, peers, padded, rest), half),
            pltpu.VMEM((ring, peers, padded, cut), half),
            pltpu.VMEM((ring, peers, padded, rest), half),
            pltpu.VMEM((items, groups, pairs, rest), half),
            pltpu.VMEM((items, groups, pairs, cut), half),
            pltpu.VMEM((items, groups, pairs, cut), half),
            pltpu.VMEM((SLOTS, groups, pairs, rest), half),
            pltpu.VMEM((SLOTS, groups, pairs, cut), half),
            pltpu.VMEM((items, groups, pairs, rest), half),
            pltpu.VMEM((items, groups, pairs, cut), half),
            pltpu.VMEM((SLOTS, groups, pairs, cut), half),
            pltpu.VMEM((2, pairs, HIGH, width), half),
            pltpu.VMEM((2, HIGH, pairs, width), half),
            dma((4, rounds, peers)), dma((4, rounds, peers)), dma((7, 2, items, groups)), dma((2,)), dma((2,)),
        ],
        compiler_params=pltpu.CompilerParams(
            collective_id=1, has_side_effects=True, vmem_limit_bytes=63 * 2**20),
    )(shift, fock, metric, active, trial)
    return outs[2], outs[5], outs[7]


def finish_kernel(groups, peers, fock_ref, trial_ref, image_ref, left_ref, rest_ref, out_ref, stats_ref,
                  trial, image, left, rest, sigma, part, slots, loaded, stored, sent, landed):
    group, me = lax.axis_index("act"), lax.axis_index("virt")
    count = groups * peers
    mine = group * peers + me
    barrier = pltpu.get_barrier_semaphore()
    chunks = loaded.shape[1]
    depth = trial.shape[0] // chunks
    rows, width = trial.shape[1], trial.shape[2]
    tail = left.shape[2]
    cut = width - tail

    def span(c):
        return pl.ds(c * depth, depth)

    def load(c, which):
        source, target = ((trial_ref, trial), (image_ref, image), (left_ref, left), (rest_ref, rest))[which]
        return pltpu.make_async_copy(source.at[span(c)], target.at[span(c)], loaded.at[which, c])

    def load_all(c, carry):
        for which in range(4):
            load(c, which).start()
        return carry

    lax.fori_loop(0, chunks, load_all, 0)

    def target(step):
        other = lax.rem(mine + step, count)
        return other, (other // peers, lax.rem(other, peers))

    def greet(step, carry):
        pl.semaphore_signal(barrier, inc=1, device_id=target(step)[1], device_id_type=MESH)
        return carry

    lax.fori_loop(1, count, greet, 0)

    def product(c, carry):
        numer, denom = carry
        for which in range(4):
            load(c, which).wait()
        own = image[span(c)].reshape(depth * rows, width)
        total = jnp.dot(own, fock_ref[...], preferred_element_type=jnp.float32)
        total += rest[span(c)].reshape(depth * rows, width).astype(jnp.float32)
        last = total[:, cut:] + left[span(c)].reshape(depth * rows, tail).astype(jnp.float32)
        total = jnp.concatenate([total[:, :cut], last], axis=1)
        sigma[span(c)] = total.reshape(depth, rows, width)
        wide = trial[span(c)].reshape(depth * rows, width).astype(jnp.float32)
        numer += jnp.sum(wide * total, axis=0, keepdims=True)
        denom += jnp.sum(wide * own.astype(jnp.float32), axis=0, keepdims=True)
        return numer, denom

    zero = jnp.zeros((1, width), jnp.float32)
    numer, denom = lax.fori_loop(0, chunks, product, (zero, zero))
    pl.semaphore_wait(barrier, count - 1)

    def sum_all(phase, value):
        part[phase] = value

        def copy(step, slot):
            other, place = target(step)
            return pltpu.make_async_remote_copy(
                src_ref=part.at[phase], dst_ref=slots.at[phase, slot],
                send_sem=sent.at[phase, other], recv_sem=landed.at[phase, slot],
                device_id=place, device_id_type=MESH)

        def send(step, carry):
            copy(step, mine).start()
            return carry

        lax.fori_loop(1, count, send, 0)
        slots[phase, mine] = value

        def receive(step, carry):
            copy(step, target(step)[0]).wait_recv()
            return carry

        lax.fori_loop(1, count, receive, 0)

        def finish(step, carry):
            copy(step, mine).wait_send()
            return carry

        lax.fori_loop(1, count, finish, 0)
        return jnp.sum(slots[phase], axis=0)

    row = lax.broadcasted_iota(jnp.int32, (8, 128), 0)
    numer_one = jnp.sum(numer, axis=1, keepdims=True)
    denom_one = jnp.sum(denom, axis=1, keepdims=True)
    sums = sum_all(0, jnp.where(row == 0, numer_one, denom_one))
    denominator = sums[1:2, 0:1]
    rayleigh = sums[0:1, 0:1] / denominator

    def store(c):
        return pltpu.make_async_copy(rest.at[span(c)], out_ref.at[span(c)], stored.at[c])

    def residual(c, squares):
        own = image[span(c)].reshape(depth * rows, width).astype(jnp.float32)
        resid = sigma[span(c)].reshape(depth * rows, width) - rayleigh * own
        rest[span(c)] = resid.astype(jnp.bfloat16).reshape(depth, rows, width)
        store(c).start()
        return squares + jnp.sum(resid * resid, axis=0, keepdims=True)

    squares = lax.fori_loop(0, chunks, residual, zero)
    square_one = jnp.sum(squares, axis=1, keepdims=True)
    norms = sum_all(1, jnp.broadcast_to(square_one, (8, 128)))
    stats_ref[...] = jnp.where(row == 0, rayleigh, norms / denominator)

    def drain(c, carry):
        store(c).wait()
        return carry

    lax.fori_loop(0, chunks, drain, 0)


def finish(groups, peers, fock, trial, image, left, rest):
    pairs, rows, width = trial.shape
    depth = next(d for d in (5, 4, 2, 1) if pairs % d == 0)
    chunks = pairs // depth
    whole = pl.BlockSpec(memory_space=pltpu.VMEM)
    anywhere = pl.BlockSpec(memory_space=pl.ANY)
    dma = pltpu.SemaphoreType.DMA
    count = groups * peers
    return pl.pallas_call(
        functools.partial(finish_kernel, groups, peers),
        out_shape=[
            jax.ShapeDtypeStruct((pairs, rows, width), jnp.bfloat16),
            jax.ShapeDtypeStruct((8, 128), jnp.float32),
        ],
        in_specs=[whole] + [anywhere] * 4,
        out_specs=[anywhere, whole],
        scratch_shapes=[
            pltpu.VMEM((pairs, rows, width), jnp.bfloat16),
            pltpu.VMEM((pairs, rows, width), jnp.bfloat16),
            pltpu.VMEM((pairs, rows, left.shape[2]), jnp.bfloat16),
            pltpu.VMEM((pairs, rows, width), jnp.bfloat16),
            pltpu.VMEM((pairs, rows, width), jnp.float32),
            pltpu.VMEM((2, 8, 128), jnp.float32),
            pltpu.VMEM((2, count, 8, 128), jnp.float32),
            dma((4, chunks)), dma((chunks,)), dma((2, count)), dma((2, count)),
        ],
        compiler_params=pltpu.CompilerParams(
            collective_id=2, has_side_effects=True, vmem_limit_bytes=63 * 2**20),
    )(fock, trial, image, left, rest)


def local(amplitudes, virtual_fock_block, metric, active_block):
    pairs, rows, width = amplitudes.shape
    peers, groups = lax.axis_size("virt"), lax.axis_size("act")
    fock = virtual_fock_block
    padded = -(-rows // 16) * 16
    room = -pairs % 8
    cut = (2 * width // 5) // 128 * 128

    def widen(array):
        if padded == rows:
            return array
        return jnp.pad(array, ((0, 0), (0, padded - rows), (0, 0)))

    def pair_matrix(array):
        spread = jnp.pad(array.reshape(groups, pairs, groups, pairs), ((0, 0), (0, room), (0, 0), (0, 0)))
        return jnp.transpose(spread, (2, 0, 1, 3)).reshape(groups, groups * (pairs + room), pairs)

    spread = fock
    if padded != rows:
        gap = padded - rows
        spread = jnp.pad(
            fock.reshape(peers, rows, peers, rows), ((0, 0), (0, gap), (0, 0), (0, gap))
        ).reshape(peers * padded, peers * padded)
    metric_parts, active_parts = pair_matrix(metric), pair_matrix(active_block)
    at = lax.broadcasted_iota(jnp.int32, fock.shape, 0)
    across = lax.broadcasted_iota(jnp.int32, fock.shape, 1)
    shift = (2.0 / width) * jnp.sum(jnp.where(at == across, fock.astype(jnp.float32), 0.0))
    trial = widen(amplitudes)
    image, left, rest = sweep(
        groups, peers, rows, cut, shift.reshape(1), spread, metric_parts, active_parts, trial)
    resid, stats = finish(groups, peers, fock, trial, image, left, rest)
    return resid[:, :rows], stats[0, 0], stats[1, 0]


def solution(mesh):
    placed = (P("act", "virt", None), P(), P(), P())
    return jax.shard_map(
        local,
        mesh=mesh,
        in_specs=placed,
        out_specs=(P("act", "virt", None), P(), P()),
        check_vma=False,
    )
```

```python
import functools

import jax
import jax.numpy as jnp
from jax import lax
from jax.experimental import pallas as pl
from jax.experimental.pallas import tpu as pltpu
from jax.sharding import PartitionSpec as P

MESH = pl.DeviceIdType.MESH
AHEAD = 4


HIGH = 16
SLOTS = 8
WINDOW = 8
EARLY = 3
JOIN = 5
MERGE = 4
TALL = 8


def main_kernel(groups, peers, rows, cut, spread_ref, metric_in, active_in, fock_ref, trial_ref,
                trial_rows, image_rows, image_ref, front_ref, front_rows, left_ref, rest_rows, rest_ref,
                sigma_ref, stats_ref,
                held_a, held_b, made_a, made_b, late_held, soon_held, front_held, late_image, soon_image,
                late_kept, soon_kept, rest_made, flat, turned, trial, image, rest, left, sigma, sums, part, slots,
                metric_ref, active_ref, shift_ref,
                sems_a, sems_b, act_sems, loaded, stored, fetched, written, sent, landed):
    group, me = lax.axis_index("act"), lax.axis_index("virt")
    pairs, padded, width = trial_ref.shape
    rounds = held_a.shape[0]
    items = rows // groups
    chunks = padded // HIGH
    per_chunk = HIGH // groups
    soon, late = pl.ds(0, cut), pl.ds(cut, width - cut)

    mine, devices = group * peers + me, groups * peers

    def target(step):
        other = lax.rem(mine + step, devices)
        return other, (other // peers, lax.rem(other, peers))

    barrier = pltpu.get_barrier_semaphore()

    def greet(step, carry):
        pl.semaphore_signal(barrier, inc=1, device_id=target(step)[1], device_id_type=MESH)
        return carry

    lax.fori_loop(1, devices, greet, 0)

    whole_rounds = pairs // peers
    spare = pairs % peers
    stride = peers // spare if spare and peers % spare == 0 else 1

    def pair_of(r, owner):
        return r * peers + owner - (r // whole_rounds) * (owner - owner // stride)

    def owns(r, owner):
        return (r // whole_rounds) * peers * lax.rem(owner, stride) + pair_of(r, owner) < pairs

    class Fock:
        def __init__(self, source, columns, held, made, target, sems):
            self.source, self.columns, self.held, self.made = source, columns, held, made
            self.target, self.sems, self.ring = target, sems, made.shape[0]

        def slab(self, t):
            return self.source.at[t, :, self.columns]

        def forward(self, r, peer):
            return pltpu.make_async_remote_copy(
                src_ref=self.slab(pair_of(r, peer)), dst_ref=self.held.at[r, me],
                send_sem=self.sems.at[0, r, peer], recv_sem=self.sems.at[1, r, me],
                device_id=(group, peer), device_id_type=MESH)

        def forward_own(self, r):
            return pltpu.make_async_copy(
                self.slab(pair_of(r, me)), self.held.at[r, me], self.sems.at[1, r, me])

        def arrival(self, r, peer):
            return pltpu.make_async_remote_copy(
                src_ref=self.held.at[r, me], dst_ref=self.held.at[r, peer],
                send_sem=self.sems.at[0, r, peer], recv_sem=self.sems.at[1, r, peer],
                device_id=(group, peer), device_id_type=MESH)

        def backward(self, r, peer):
            return pltpu.make_async_remote_copy(
                src_ref=self.made.at[lax.rem(r, self.ring), peer], dst_ref=self.target.at[pair_of(r, me)],
                send_sem=self.sems.at[2, r, peer], recv_sem=self.sems.at[3, r, me],
                device_id=(group, peer), device_id_type=MESH)

        def backward_own(self, r):
            return pltpu.make_async_copy(
                self.made.at[lax.rem(r, self.ring), me], self.target.at[pair_of(r, me)], self.sems.at[3, r, me])

        def back_arrival(self, r, peer):
            return pltpu.make_async_remote_copy(
                src_ref=self.made.at[0, peer], dst_ref=self.target.at[pair_of(r, peer)],
                send_sem=self.sems.at[2, r, peer], recv_sem=self.sems.at[3, r, peer],
                device_id=(group, peer), device_id_type=MESH)

        def launch(self, r):
            for step in range(peers):
                peer = lax.rem(me + step, peers)

                @pl.when(owns(r, peer))
                def _(step=step, peer=peer):
                    if step == 0:
                        self.forward_own(r).start()
                    else:
                        self.forward(r, peer).start()

        def launch_first(self):
            def ahead(r, carry):
                self.launch(r)
                return carry

            lax.fori_loop(0, min(AHEAD, rounds), ahead, 0)

        def launch_next(self, r):
            @pl.when(r + AHEAD < rounds)
            def _():
                self.launch(r + AHEAD)

        def sent_back(self, r):
            for step in range(1, peers):
                self.backward(r, lax.rem(me + step, peers)).wait_send()

        def apply(self, r):
            @pl.when(r >= 1)
            def _():
                self.backward_own(r - 1).wait()

            @pl.when(owns(r, me))
            def _():
                self.forward_own(r).wait()
                for step in range(1, peers):
                    self.arrival(r, lax.rem(me + step, peers)).wait_recv()

                @pl.when(r >= self.ring)
                def _():
                    self.sent_back(r - self.ring)

                block = self.held[r].reshape(peers * padded, self.held.shape[3])
                product = jnp.dot(spread_ref[...], block, preferred_element_type=jnp.float32)
                self.made[lax.rem(r, self.ring)] = product.astype(jnp.bfloat16).reshape(
                    peers, padded, self.held.shape[3])
                self.backward_own(r).start()
                for step in range(1, peers):
                    self.backward(r, lax.rem(me + step, peers)).start()

        def settle_own(self):
            @pl.when(owns(rounds - 1, me))
            def _():
                self.backward_own(rounds - 1).wait()

        def settle(self, r):
            for step in range(1, peers):
                peer = lax.rem(me + step, peers)

                @pl.when(owns(r, peer))
                def _(peer=peer):
                    self.back_arrival(r, peer).wait_recv()

        def drain(self):
            def done(r, carry):
                for step in range(1, peers):
                    peer = lax.rem(me + step, peers)

                    @pl.when(owns(r, peer))
                    def _(peer=peer):
                        self.forward(r, peer).wait_send()

                return carry

            lax.fori_loop(0, rounds, done, 0)

            def back_done(r, carry):
                kept = (r + self.ring < rounds - 1) | ((r + self.ring == rounds - 1) & owns(rounds - 1, me))

                @pl.when(owns(r, me) & jnp.logical_not(kept))
                def _():
                    self.sent_back(r)

                return carry

            lax.fori_loop(0, rounds, back_done, 0)

    class Swap:
        def __init__(self, kind, source, target):
            self.kind, self.source, self.target = kind, source, target

        def send(self, i, peer):
            return pltpu.make_async_remote_copy(
                src_ref=self.source(i, peer), dst_ref=self.target(i, group),
                send_sem=act_sems.at[self.kind, 0, i, peer], recv_sem=act_sems.at[self.kind, 1, i, group],
                device_id=(peer, me), device_id_type=MESH)

        def own(self, i):
            return pltpu.make_async_copy(
                self.source(i, group), self.target(i, group), act_sems.at[self.kind, 1, i, group])

        def arrival(self, i, peer):
            return pltpu.make_async_remote_copy(
                src_ref=self.source(i, peer), dst_ref=self.target(i, peer),
                send_sem=act_sems.at[self.kind, 0, i, peer], recv_sem=act_sems.at[self.kind, 1, i, peer],
                device_id=(peer, me), device_id_type=MESH)

        def start(self, i):
            self.own(i).start()
            for step in range(1, groups):
                self.send(i, lax.rem(group + step, groups)).start()

        def wait_remote(self, i):
            for step in range(1, groups):
                self.arrival(i, lax.rem(group + step, groups)).wait_recv()

        def wait(self, i):
            self.own(i).wait()
            self.wait_remote(i)

        def sent(self, i):
            for step in range(1, groups):
                self.send(i, lax.rem(group + step, groups)).wait_send()

        def drain(self, first):
            def done(i, carry):
                self.sent(i)
                return carry

            lax.fori_loop(first, items, done, 0)

    def row(i, owner):
        return i * groups + owner

    def slot(i):
        return lax.rem(i, SLOTS)

    front = Fock(trial_ref, soon, held_a, made_a, front_ref, sems_a)
    back = Fock(image_ref, late, held_b, made_b, left_ref, sems_b)
    late_in = Swap(0, lambda i, p: trial_rows.at[row(i, p), :, late], lambda i, p: late_held.at[i, p])
    soon_in = Swap(1, lambda i, p: trial_rows.at[row(i, p), :, soon], lambda i, p: soon_held.at[i, p])
    late_out = Swap(2, lambda i, p: late_image.at[slot(i), p], lambda i, p: image_rows.at[row(i, p), :, late])
    soon_out = Swap(3, lambda i, p: soon_image.at[slot(i), p], lambda i, p: image_rows.at[row(i, p), :, soon])
    kept_out = Swap(4, lambda i, p: late_kept.at[i, p], lambda i, p: rest_rows.at[row(i, p), :, late])
    front_in = Swap(5, lambda i, p: front_rows.at[row(i, p)], lambda i, p: front_held.at[i, p])
    rest_out = Swap(6, lambda i, p: rest_made.at[slot(i), p], lambda i, p: rest_rows.at[row(i, p), :, soon])

    def run(low, high, work):
        def one(i, carry):
            work(i)
            return carry

        lax.fori_loop(low, high, one, 0)

    def strip(c):
        return pl.ds(pl.multiple_of(c * HIGH, HIGH), HIGH)

    def blocks(extent, work):
        def one(j, carry):
            work(pl.ds(pl.multiple_of(j * 128, 128), 128))
            return carry

        lax.fori_loop(0, extent // 128, one, 0)

    def to_rows(at, extent):
        def work(columns):
            turned[at, :, :, columns] = jnp.transpose(flat[at, :, :, columns], (1, 0, 2))

        blocks(extent, work)

    def to_flat(c, at, extent):
        def work(columns):
            block = jnp.transpose(turned[at, :, :, columns], (1, 0, 2))
            if padded != rows:
                place = c * HIGH + lax.broadcasted_iota(jnp.int32, block.shape, 1)
                block = jnp.where(place < rows, block, jnp.zeros_like(block))
            flat[at, :, :, columns] = block

        blocks(extent, work)

    def turn_back(c, source, target, columns, extent):
        load = pltpu.make_async_copy(
            source.at[strip(c), :, columns], turned.at[0, :, :, pl.ds(0, extent)], loaded.at[0])
        load.start()
        load.wait()
        to_flat(c, 0, extent)
        store = pltpu.make_async_copy(
            flat.at[0, :, :, pl.ds(0, extent)], target.at[:, strip(c), columns], stored.at[0])
        store.start()
        store.wait()

    def arrived(swap, c, work):
        run(c * per_chunk, jnp.minimum((c + 1) * per_chunk, items), work)

    def image_late(c):
        arrived(late_out, c, late_out.wait_remote)
        turn_back(c, image_rows, image_ref, late, width - cut)

    def image_soon(c):
        arrived(soon_out, c, soon_out.wait_remote)
        turn_back(c, image_rows, image_ref, soon, cut)

    def rest_late(c):
        arrived(kept_out, c, kept_out.wait)
        turn_back(c, rest_rows, rest_ref, late, width - cut)

    def rest_soon(c):
        arrived(rest_out, c, rest_out.wait_remote)
        turn_back(c, rest_rows, rest_ref, soon, cut)

    def mix(matrix_ref, held, i):
        total = jnp.dot(matrix_ref[0], held[i, 0], preferred_element_type=jnp.float32)
        for q in range(1, groups):
            total += jnp.dot(matrix_ref[q], held[i, q], preferred_element_type=jnp.float32)
        return total.reshape(groups, -1, total.shape[1])[:, :pairs]

    def settled(swap, i):
        @pl.when(i >= 1)
        def _():
            swap.own(i - 1).wait()

        @pl.when(i >= SLOTS)
        def _():
            swap.sent(i - SLOTS)

    def closed(swap, i):
        @pl.when(i == items - 1)
        def _():
            swap.own(i).wait()

    def weigh(i, taken, given, held, image, kept):
        taken.wait(i)
        settled(given, i)

        weighted = mix(metric_ref, held, i)
        half = weighted.astype(jnp.bfloat16)
        image[slot(i)] = half
        given.start(i)
        active = mix(active_ref, held, i) - shift_ref[...] * (weighted - half.astype(jnp.float32))
        kept[i] = active.astype(kept.dtype)
        closed(given, i)

    def feed(j):
        @pl.when(j < items)
        def _():
            late_in.start(j)

        @pl.when((j >= items) & (j < 2 * items))
        def _():
            soon_in.start(j - items)

    def weigh_late(i):
        feed(i + WINDOW)
        weigh(i, late_in, late_out, late_held, late_image, late_kept)

    def weigh_soon(i):
        feed(items + i + WINDOW)
        weigh(i, soon_in, soon_out, soon_held, soon_image, soon_kept)
        kept_out.start(i)

    def combine(i):
        @pl.when(i + WINDOW < items)
        def _():
            front_in.start(i + WINDOW)

        front_in.wait(i)
        settled(rest_out, i)

        total = soon_kept[i].astype(jnp.float32) + mix(metric_ref, front_held, i)
        rest_made[slot(i)] = total.astype(jnp.bfloat16)
        rest_out.start(i)
        closed(rest_out, i)

    def load_trial(c):
        return pltpu.make_async_copy(trial_ref.at[:, strip(c), :], flat.at[lax.rem(c, 2)], loaded.at[lax.rem(c, 2)])

    def store_rows(c):
        return pltpu.make_async_copy(turned.at[lax.rem(c, 2)], trial_rows.at[strip(c)], stored.at[lax.rem(c, 2)])

    def turn_trial(c):
        @pl.when(c < chunks)
        def _():
            load_trial(c).wait()
            to_rows(lax.rem(c, 2), width)
            store_rows(c).start()

        @pl.when(c + 2 < chunks)
        def _():
            load_trial(c + 2).start()

        @pl.when(c >= 1)
        def _():
            store_rows(c - 1).wait()
            run((c - 1) * per_chunk, jnp.minimum(c * per_chunk, min(WINDOW, items)), late_in.start)

    def turn_front(c):
        load = pltpu.make_async_copy(
            front_ref.at[:, strip(c), :], flat.at[0, :, :, soon], loaded.at[0])
        load.start()
        load.wait()
        to_rows(0, cut)
        store = pltpu.make_async_copy(turned.at[0, :, :, soon], front_rows.at[strip(c)], stored.at[0])
        store.start()
        store.wait()

    depth = trial.shape[1]
    spans = pairs // depth

    def span(c):
        return pl.ds(c * depth, depth)

    def fetches(c):
        at = lax.rem(c, 2)
        return [
            pltpu.make_async_copy(source.at[span(c)], place.at[at], fetched.at[which, at])
            for which, (source, place) in enumerate(
                ((trial_ref, trial), (image_ref, image), (rest_ref, rest)))]

    def fetch_left(c):
        at = lax.rem(c, 2)
        return pltpu.make_async_copy(left_ref.at[span(c)], left.at[at], fetched.at[3, at])

    def write(c):
        at = lax.rem(c, 2)
        return pltpu.make_async_copy(sigma.at[at], sigma_ref.at[span(c)], written.at[at])

    def total(value):
        return jnp.sum(value, axis=0, keepdims=True)

    def join(c):
        at = lax.rem(c, 2)

        @pl.when(lax.rem(c * depth, peers) == 0)
        def _():
            back.settle(c * depth // peers)

        fetch_left(c).start()

        @pl.when(c + 1 < spans)
        def _():
            for copy in fetches(c + 1):
                copy.start()

        for copy in fetches(c):
            copy.wait()

        @pl.when(c >= 2)
        def _():
            write(c - 2).wait()

        own = image[at].reshape(depth * padded, width)
        sums_of = jnp.dot(own, fock_ref[...], preferred_element_type=jnp.float32)
        sums_of += rest[at].reshape(depth * padded, width).astype(jnp.float32)
        fetch_left(c).wait()
        tail = sums_of[:, cut:] + left[at].reshape(depth * padded, width - cut).astype(jnp.float32)
        sums_of = jnp.concatenate([sums_of[:, :cut], tail], axis=1)
        own = own.astype(jnp.float32)
        wide = trial[at].reshape(depth * padded, width).astype(jnp.float32)
        apart = sums_of - shift_ref[...] * own
        sigma[at] = apart.astype(jnp.bfloat16).reshape(depth, padded, width)
        write(c).start()
        sums[0:1] += total(wide * apart)
        sums[1:2] += total(wide * own)
        sums[2:3] += total(apart * apart)
        sums[3:4] += total(apart * own)
        sums[4:5] += total(own * own)

    def gather(value):
        part[...] = value

        def copy(step, at):
            other, place = target(step)
            return pltpu.make_async_remote_copy(
                src_ref=part, dst_ref=slots.at[at], send_sem=sent.at[other], recv_sem=landed.at[at],
                device_id=place, device_id_type=MESH)

        def send(step, carry):
            copy(step, mine).start()
            return carry

        lax.fori_loop(1, devices, send, 0)
        slots[mine] = value

        def receive(step, carry):
            copy(step, target(step)[0]).wait_recv()
            return carry

        lax.fori_loop(1, devices, receive, 0)

        def done(step, carry):
            copy(step, mine).wait_send()
            return carry

        lax.fori_loop(1, devices, done, 0)
        return jnp.sum(slots[...], axis=0)

    def finish():
        sums[...] = jnp.zeros_like(sums)
        for copy in fetches(0):
            copy.start()
        run(0, spans, join)
        found = jnp.sum(sums[...], axis=1, keepdims=True)
        found = gather(jnp.broadcast_to(found, (8, 128)))
        denominator = found[1:2]
        over = found[0:1] / denominator
        squares = found[2:3] - 2.0 * over * found[3:4] + over * over * found[4:5]
        at = lax.broadcasted_iota(jnp.int32, (8, 128), 0)
        stats_ref[...] = jnp.where(
            at == 0, shift_ref[...] + over, jnp.where(at == 1, squares / denominator, over))
        for c in range(max(spans - 2, 0), spans):
            write(c).wait()

    def prepare():
        tall = metric_ref.shape[1] // groups
        for source, place in ((metric_in, metric_ref), (active_in, active_ref)):
            place[...] = jnp.zeros_like(place)
            for q in range(groups):
                for p in range(groups):
                    place[q, pl.ds(p * tall, pairs), :] = source[pl.ds(p * pairs, pairs), pl.ds(q * pairs, pairs)]
        at = lax.broadcasted_iota(jnp.int32, fock_ref.shape, 0)
        across = lax.broadcasted_iota(jnp.int32, fock_ref.shape, 1)
        diagonal = jnp.where(at == across, fock_ref[...].astype(jnp.float32), 0.0)
        shift_ref[...] = (2.0 / width) * jnp.sum(jnp.sum(diagonal, axis=0, keepdims=True), axis=1, keepdims=True)

    def count(value, most):
        return jnp.clip(value, 0, most)

    for c in range(min(2, chunks)):
        load_trial(c).start()
    pl.semaphore_wait(barrier, devices - 1)
    front.launch_first()
    run(0, chunks + 1, turn_trial)
    prepare()
    run(items, WINDOW, feed)

    late_ticks = max(1, rounds - 2)

    def weighed_late(r):
        return count(((r + 1) * items + late_ticks // 2) // late_ticks, items)

    def image_done(r):
        ready = jnp.where(r >= 1, weighed_late(r - 1), 0)
        return jnp.where(ready == items, chunks, ready // per_chunk)

    def weighed_early(r):
        return count((r + 2 - rounds) * EARLY, items)

    def first_tick(r):
        front.launch_next(r)
        run(weighed_late(r - 1), weighed_late(r), weigh_late)
        run(weighed_early(r - 1), weighed_early(r), weigh_soon)
        run(image_done(r - 1), image_done(r), image_late)

        @pl.when(r == rounds - 1)
        def _():
            run(image_done(r), chunks, image_late)
            back.launch_first()

        front.apply(r)

    run(0, rounds, first_tick)
    begun = weighed_early(rounds - 1)

    def weighed_soon(r):
        return count(begun + (r + 1) * EARLY, items)

    def combined(r):
        return count((r + 1 - JOIN) * MERGE, items)

    def soon_done(r):
        return count(jnp.where(weighed_soon(r - 1) == items, chunks, weighed_soon(r - 1) // per_chunk), chunks)

    def late_done(r):
        return jnp.where(r >= 1, soon_done(r - 1), 0)

    def rest_done(r):
        return combined(r - 1) // per_chunk

    def second_tick(r):
        back.launch_next(r)
        run(weighed_soon(r - 1), weighed_soon(r), weigh_soon)

        @pl.when(r == 1)
        def _():
            front.settle_own()
            run(0, rounds, front.settle)
            run(0, chunks, turn_front)
            run(0, min(WINDOW, items), front_in.start)

        run(combined(r - 1), combined(r), combine)
        run(soon_done(r - 1), soon_done(r), image_soon)
        run(late_done(r - 1), late_done(r), rest_late)
        run(rest_done(r - 1), rest_done(r), rest_soon)
        back.apply(r)

    run(0, rounds, second_tick)
    last = rounds - 1
    run(weighed_soon(last), items, weigh_soon)
    run(soon_done(last), chunks, image_soon)
    run(late_done(last), chunks, rest_late)
    most = min(items, (chunks - 1) * per_chunk + 1)
    run(combined(last), most, combine)
    run(rest_done(last), chunks - 1, rest_soon)
    run(jnp.maximum(combined(last), most), items, combine)
    run(jnp.maximum(rest_done(last), chunks - 1), chunks, rest_soon)
    back.settle_own()
    finish()
    front.drain()
    back.drain()
    late_in.drain(0)
    soon_in.drain(0)
    kept_out.drain(0)
    front_in.drain(0)
    for swap in (late_out, soon_out, rest_out):
        swap.drain(max(items - SLOTS, 0))


def sweep(groups, peers, rows, cut, spread, metric, active, fock, trial):
    pairs, padded, width = trial.shape
    items = rows // groups
    rounds = -(-pairs // peers)
    rest = width - cut
    ring = min(rounds, 6)
    devices, tall = groups * peers, -(-pairs // TALL) * TALL
    depth = next(d for d in (4, 2, 1) if pairs % d == 0 and peers % d == 0)
    whole = pl.BlockSpec(memory_space=pltpu.VMEM)
    anywhere = pl.BlockSpec(memory_space=pl.ANY)
    half, dma = jnp.bfloat16, pltpu.SemaphoreType.DMA

    def made(*shape):
        return jax.ShapeDtypeStruct(shape, half)

    outs = pl.pallas_call(
        functools.partial(main_kernel, groups, peers, rows, cut),
        out_shape=[
            made(padded, pairs, width), made(padded, pairs, width), made(pairs, padded, width),
            made(pairs, padded, cut), made(padded, pairs, cut), made(pairs, padded, rest),
            made(padded, pairs, width), made(pairs, padded, width),
            made(pairs, padded, width),
            jax.ShapeDtypeStruct((8, 128), jnp.float32),
        ],
        in_specs=[whole] * 4 + [anywhere],
        out_specs=[anywhere] * 9 + [whole],
        scratch_shapes=[
            pltpu.VMEM((rounds, peers, padded, cut), half),
            pltpu.VMEM((rounds, peers, padded, rest), half),
            pltpu.VMEM((ring, peers, padded, cut), half),
            pltpu.VMEM((ring, peers, padded, rest), half),
            pltpu.VMEM((items, groups, pairs, rest), half),
            pltpu.VMEM((items, groups, pairs, cut), half),
            pltpu.VMEM((items, groups, pairs, cut), half),
            pltpu.VMEM((SLOTS, groups, pairs, rest), half),
            pltpu.VMEM((SLOTS, groups, pairs, cut), half),
            pltpu.VMEM((items, groups, pairs, rest), half),
            pltpu.VMEM((items, groups, pairs, cut), half),
            pltpu.VMEM((SLOTS, groups, pairs, cut), half),
            pltpu.VMEM((2, pairs, HIGH, width), half),
            pltpu.VMEM((2, HIGH, pairs, width), half),
            pltpu.VMEM((2, depth, padded, width), half),
            pltpu.VMEM((2, depth, padded, width), half),
            pltpu.VMEM((2, depth, padded, width), half),
            pltpu.VMEM((2, depth, padded, rest), half),
            pltpu.VMEM((2, depth, padded, width), half),
            pltpu.VMEM((8, width), jnp.float32),
            pltpu.VMEM((8, 128), jnp.float32),
            pltpu.VMEM((devices, 8, 128), jnp.float32),
            pltpu.VMEM((groups, groups * tall, pairs), half),
            pltpu.VMEM((groups, groups * tall, pairs), half),
            pltpu.VMEM((1, 1), jnp.float32),
            dma((4, rounds, peers)), dma((4, rounds, peers)), dma((7, 2, items, groups)), dma((2,)), dma((2,)),
            dma((4, 2)), dma((2,)), dma((devices,)), dma((devices,)),
        ],
        compiler_params=pltpu.CompilerParams(
            collective_id=1, has_side_effects=True, vmem_limit_bytes=63 * 2**20),
    )(spread, metric, active, fock, trial)
    return outs[2], outs[8], outs[9]


def close_kernel(stats_ref, apart_ref, image_ref, out_ref, apart, image, loaded, stored):
    chunks = loaded.shape[1]
    depth = apart.shape[0] // chunks
    over = stats_ref[2:3, 0:1].reshape(1, 1, 1)

    def span(c):
        return pl.ds(c * depth, depth)

    def loads(c):
        return (pltpu.make_async_copy(apart_ref.at[span(c)], apart.at[span(c)], loaded.at[0, c]),
                pltpu.make_async_copy(image_ref.at[span(c)], image.at[span(c)], loaded.at[1, c]))

    def store(c):
        return pltpu.make_async_copy(apart.at[span(c)], out_ref.at[span(c)], stored.at[c])

    def begin(c, carry):
        for copy in loads(c):
            copy.start()
        return carry

    def close_one(c, carry):
        for copy in loads(c):
            copy.wait()
        resid = apart[span(c)].astype(jnp.float32) - over * image[span(c)].astype(jnp.float32)
        apart[span(c)] = resid.astype(apart.dtype)
        store(c).start()
        return carry

    def end(c, carry):
        store(c).wait()
        return carry

    for work in (begin, close_one, end):
        lax.fori_loop(0, chunks, work, 0)


def close(stats, apart, image):
    pairs, padded, width = apart.shape
    depth = next(d for d in (5, 4, 2, 1) if pairs % d == 0)
    anywhere = pl.BlockSpec(memory_space=pl.ANY)
    dma = pltpu.SemaphoreType.DMA
    return pl.pallas_call(
        close_kernel,
        out_shape=jax.ShapeDtypeStruct(image.shape, image.dtype),
        in_specs=[pl.BlockSpec(memory_space=pltpu.VMEM), anywhere, anywhere],
        out_specs=anywhere,
        scratch_shapes=[
            pltpu.VMEM(apart.shape, apart.dtype), pltpu.VMEM(image.shape, image.dtype),
            dma((2, pairs // depth)), dma((pairs // depth,)),
        ],
        compiler_params=pltpu.CompilerParams(vmem_limit_bytes=60 * 2**20),
    )(stats, apart, image)


def local(amplitudes, virtual_fock_block, metric, active_block):
    pairs, rows, width = amplitudes.shape
    peers, groups = lax.axis_size("virt"), lax.axis_size("act")
    fock = virtual_fock_block
    padded = -(-rows // 16) * 16
    cut = (2 * width // 5) // 128 * 128

    def widen(array):
        if padded == rows:
            return array
        return jnp.pad(array, ((0, 0), (0, padded - rows), (0, 0)))

    spread = fock
    if padded != rows:
        gap = padded - rows
        spread = jnp.pad(
            fock.reshape(peers, rows, peers, rows), ((0, 0), (0, gap), (0, 0), (0, gap))
        ).reshape(peers * padded, peers * padded)
    trial = widen(amplitudes)
    image, sigma, stats = sweep(
        groups, peers, rows, cut, spread, metric, active_block, fock, trial)
    resid = close(stats, sigma, image)
    return resid[:, :rows], stats[0, 0], stats[1, 0]


def solution(mesh):
    placed = (P("act", "virt", None), P(), P(), P())
    return jax.shard_map(
        local,
        mesh=mesh,
        in_specs=placed,
        out_specs=(P("act", "virt", None), P(), P()),
        check_vma=False,
    )
```
